32 devices in a mesh: dp: 8 (over z, y), seq: 4 (over x, core).
Axes of the slice: x: 2, y: 2, z: 4, core: 2. Of those that a mesh axis runs over, the one named last changes fastest.
Arguments:
- queries: bfloat16 [8, 512, 2048], P('dp', 'seq'), may hold values from -5 to 5
- keys: bfloat16 [8, 512, 2048], P('dp', 'seq'), may hold values from -5 to 5
- values: bfloat16 [8, 512, 2048], P('dp', 'seq'), may hold values from -6 to 6
- stream: bfloat16 [8, 512, 2048], P('dp', 'seq'), may hold values from -40 to 40
- layer_scale: float32 [2048], replicated, may hold values from 0.5 to 2
- norm_gain: float32 [2048], replicated, may hold values from 0.5 to 2
- teacher_gram: bfloat16 [8, 512, 512], P('dp', 'seq'), may hold values from -20 to 20, as said below
Outputs:
- feature_grad: bfloat16 [8, 512, 2048], P('dp', 'seq')
- image_loss: float32 [8], P('dp')
- mean_loss: float32 [], replicated
The draws below stay inside these ranges and needn't reach their ends.
Inputs may be any that keep to these rules, and one draw needn't show every extreme that they name: Each image's teacher_gram is symmetric.
All inputs are finite; a program needn't handle non-finite values.
Results may differ from the reference program's by a relative error of at most 0.009.
Values may be sent and summed in bfloat16 or wider, within the bound.
A program may use at most 64 MiB of HBM per device.

```python
import math
import jax
import jax.numpy as jnp
from jax import lax

HEADS = 32
HEAD_DIM = 64
WIDTH = 2048
TOKENS = 512
IMAGES = 8


def query_key_pair(key):
    first_key = jax.random.fold_in(key, 101)
    second_key = jax.random.fold_in(key, 102)
    full_shape = (IMAGES, TOKENS, WIDTH)
    query_draw = 1.4 * jax.random.truncated_normal(first_key, -3.5, 3.5, full_shape, jnp.float32)
    key_draw = 1.4 * jax.random.truncated_normal(second_key, -3.5, 3.5, full_shape, jnp.float32)
    return (query_draw, key_draw)


def draw_queries(key, part):
    return query_key_pair(key)[0].astype(jnp.bfloat16)


def draw_keys(key, part):
    return query_key_pair(key)[1].astype(jnp.bfloat16)


def draw_stream(key, part):
    full_shape = (IMAGES, TOKENS, WIDTH)
    noise_key = jax.random.fold_in(key, 301)
    drawn = 0.2 * jax.random.truncated_normal(noise_key, -6.0, 6.0, full_shape, jnp.float32)
    return drawn.astype(jnp.bfloat16)


def draw_teacher_gram(key, part):
    noise_key = jax.random.fold_in(key, 201)
    full_shape = (IMAGES, TOKENS, TOKENS)
    position = jnp.arange(TOKENS, dtype=jnp.float32) / (TOKENS - 1)
    image_frac = jnp.arange(IMAGES, dtype=jnp.float32) / max(IMAGES - 1, 1)
    noise = jax.random.normal(noise_key, full_shape, jnp.float32)
    token_factor = jnp.sqrt(1.0 + 2.0 * position)
    symmetric = (noise + jnp.swapaxes(noise, 1, 2)) * (0.7071 / math.sqrt(WIDTH))
    row_factor = token_factor[None, :] * jnp.sqrt(jnp.sqrt(1.0 + 2.0 * image_frac))[:, None]
    gram = row_factor[:, :, None] * row_factor[:, None, :] * (symmetric + jnp.eye(TOKENS, dtype=jnp.float32)[None])
    return gram.astype(jnp.bfloat16)


def level_of(key, extent, pieces, low, high):
    gain = 1.0
    for dim, parts in pieces:
        draws = jax.random.uniform(jax.random.fold_in(jax.random.fold_in(key, 6), dim), (parts,), jnp.float32, low / len(pieces), high / len(pieces))
        gain = gain * jnp.repeat(jnp.exp(draws), extent[dim] // parts).reshape((-1,) + (1,) * (len(extent) - 1 - dim))
    return gain


def bell_draw(stream_key, dims, spread, bound, split=(), kind=jnp.bfloat16):
    loudness = level_of(stream_key, dims, split, -0.22, 0.18) if split else 1.0
    result = jax.random.normal(stream_key, dims, jnp.float32) * spread * loudness
    return jnp.minimum(jnp.maximum(result, -bound), bound).astype(kind)


def setup_inputs(seed: int = 0) -> dict:
    seeds = jax.random.split(jax.random.key(seed), 8)
    return {
        "queries": draw_queries(jax.random.fold_in(seeds[7], 71), 0),
        "keys": draw_keys(jax.random.fold_in(seeds[7], 71), 0),
        "values": bell_draw(seeds[2], (IMAGES, TOKENS, WIDTH), 1.0, 6.0, ((0, 8), (1, 4))),
        "stream": draw_stream(jax.random.fold_in(seeds[7], 71), 0),
        "layer_scale": jnp.clip(jnp.exp(jax.random.uniform(seeds[4], (WIDTH,), jnp.float32, math.log(0.5), math.log(2.0))), 0.5, 2.0),
        "norm_gain": jnp.clip(jnp.exp(jax.random.uniform(seeds[5], (WIDTH,), jnp.float32, math.log(0.5), math.log(2.0))), 0.5, 2.0),
        "teacher_gram": draw_teacher_gram(jax.random.fold_in(seeds[7], 71), 0),
    }


EPSILON = 1e-06

def attend_block(q_block, k_head, v_head):
    scores = jnp.einsum('qd,kd->qk', q_block, k_head, preferred_element_type=jnp.float32) / math.sqrt(q_block.shape[1])
    row_max = lax.optimization_barrier(jnp.max(scores, axis=1, keepdims=True))
    exponent = jnp.exp(scores - row_max)
    weights = (exponent / lax.optimization_barrier(jnp.sum(exponent, axis=1, keepdims=True))).astype(jnp.bfloat16)
    return jnp.dot(weights, v_head, preferred_element_type=jnp.float32).astype(jnp.bfloat16)

def attend_head(q_head, k_head, v_head):
    row_count, head_depth = q_head.shape
    block_rows = math.gcd(row_count, 512)
    blocks = q_head.reshape(row_count // block_rows, block_rows, head_depth)
    results = lax.map(lambda q_block: attend_block(q_block, k_head, v_head), blocks)
    return results.reshape(row_count, head_depth)

def forward_norm(summed, norm_gain):
    row_mean = lax.optimization_barrier(jnp.mean(summed, axis=-1, keepdims=True))
    centred = summed - row_mean
    variance = lax.optimization_barrier(jnp.mean(centred * centred, axis=-1, keepdims=True))
    inv_sigma = lax.rsqrt(variance + EPSILON)
    centred_hat = centred * inv_sigma
    normed = centred_hat * norm_gain
    inv_length = lax.rsqrt(lax.optimization_barrier(jnp.sum(normed * normed, axis=-1, keepdims=True)) + EPSILON)
    return (centred_hat, inv_sigma, normed, inv_length)

def backward_norm(cotangent, centred_hat, inv_sigma, normed, inv_length, norm_gain):
    along = lax.optimization_barrier(jnp.sum(normed * cotangent, axis=-1, keepdims=True))
    grad_normed = inv_length * cotangent - inv_length * inv_length * inv_length * normed * along
    scaled = grad_normed * norm_gain
    mean_scaled = lax.optimization_barrier(jnp.mean(scaled, axis=-1, keepdims=True))
    mean_product = lax.optimization_barrier(jnp.mean(scaled * centred_hat, axis=-1, keepdims=True))
    return (scaled - mean_scaled - centred_hat * mean_product) * inv_sigma

def one_image(inputs, layer_scale, norm_gain):
    image_q, image_k, image_v, image_stream, image_teacher = inputs
    split_q = jnp.transpose(image_q.reshape(TOKENS, HEADS, HEAD_DIM), (1, 0, 2))
    split_k = jnp.transpose(image_k.reshape(TOKENS, HEADS, HEAD_DIM), (1, 0, 2))
    split_v = jnp.transpose(image_v.reshape(TOKENS, HEADS, HEAD_DIM), (1, 0, 2))
    per_head = lax.map(lambda triple: attend_head(triple[0], triple[1], triple[2]), (split_q, split_k, split_v))
    attended = jnp.transpose(per_head, (1, 0, 2)).reshape(TOKENS, WIDTH)
    summed = image_stream.astype(jnp.float32) + layer_scale * attended.astype(jnp.float32)
    centred_hat, inv_sigma, normed, inv_length = forward_norm(summed, norm_gain)
    features = (normed * inv_length).astype(jnp.bfloat16)
    gram_diff = jnp.einsum('ad,bd->ab', features, features, preferred_element_type=jnp.float32) - image_teacher.astype(jnp.float32)
    image_loss = jnp.sum(gram_diff * gram_diff) * (WIDTH / (TOKENS * TOKENS))
    cotangent = jnp.dot(gram_diff.astype(jnp.bfloat16), features, preferred_element_type=jnp.float32) * (4.0 * WIDTH / (TOKENS * TOKENS))
    grad_summed = backward_norm(cotangent, centred_hat, inv_sigma, normed, inv_length, norm_gain)
    feature_grad = (grad_summed * (TOKENS * math.sqrt(WIDTH))).astype(jnp.bfloat16)
    return (feature_grad, image_loss)

def reference(queries, keys, values, stream, layer_scale, norm_gain, teacher_gram):
    feature_grad, image_loss = lax.map(lambda inputs: one_image(inputs, layer_scale, norm_gain), (queries, keys, values, stream, teacher_gram))
    mean_loss = jnp.mean(image_loss)
    return (feature_grad, image_loss, mean_loss)
```

```python
import functools
import math

import jax
import jax.numpy as jnp
from jax import lax
from jax.experimental import pallas as pl
from jax.experimental.pallas import tpu as pltpu
from jax.sharding import PartitionSpec as P

HEAD_DIM = 64
EPSILON = 1e-06
LANES = 128
CORES = 2
MESH = pl.DeviceIdType.MESH
NT = (((1,), (1,)), ((), ()))
TN = (((0,), (0,)), ((), ()))


def kernel(
    seq_size,
    dp_size,
    chunk_count,
    slab_count,
    q_hbm,
    k_hbm,
    v_hbm,
    stream_hbm,
    scale_hbm,
    gain_hbm,
    teacher_hbm,
    grad_ref,
    image_ref,
    mean_ref,
    q_buf,
    kv_buf,
    stream_buf,
    scale_buf,
    gain_buf,
    teacher_buf,
    taught_t,
    hat_buf,
    feat_buf,
    cot_buf,
    stats,
    loss_acc,
    loss_seq,
    loss_dp,
    local_sem,
    kv_send,
    kv_recv,
    pair_send,
    pair_recv,
    relay_send,
    relay_recv,
    feat_send,
    feat_recv,
    fpair_send,
    fpair_recv,
    frelay_send,
    frelay_recv,
    lseq_send,
    lseq_recv,
    ldp_send,
    ldp_recv,
):
    rows, width = q_buf.shape
    chips = seq_size // CORES
    others = chips - 1
    tokens = rows * seq_size
    cols = width // chunk_count
    slab = rows // slab_count
    me = lax.axis_index("seq")
    image = lax.axis_index("dp")
    core = lax.rem(me, CORES)
    chip = me // CORES
    partner = chip * CORES + (1 - core)

    def far(d):
        return lax.rem(chip + d, chips) * CORES + core

    def source(d):
        return lax.rem(chip + chips - d, chips) * CORES + core

    def source_pair(d):
        return lax.rem(chip + chips - d, chips) * CORES + (1 - core)

    inputs = (k_hbm, v_hbm)
    locals_ = [
        pltpu.make_async_copy(src, dst, local_sem.at[i])
        for i, (src, dst) in enumerate(
            (
                (q_hbm.at[0], q_buf),
                (k_hbm.at[0], kv_buf.at[0, me]),
                (v_hbm.at[0], kv_buf.at[1, me]),
                (stream_hbm.at[0], stream_buf),
                (scale_hbm, scale_buf),
                (gain_hbm, gain_buf),
                (teacher_hbm.at[0], teacher_buf),
            )
        )
    ]

    barrier = pltpu.get_barrier_semaphore()

    def greet_seq(i, carry):
        pl.semaphore_signal(barrier, inc=1, device_id={"seq": lax.rem(me + i, seq_size)}, device_id_type=MESH)
        return carry

    def greet_dp(i, carry):
        pl.semaphore_signal(barrier, inc=1, device_id={"dp": lax.rem(image + i, dp_size)}, device_id_type=MESH)
        return carry

    lax.fori_loop(1, seq_size, greet_seq, 0)
    lax.fori_loop(1, dp_size, greet_dp, 0)
    for copy in locals_:
        copy.start()
    pl.semaphore_wait(barrier, seq_size + dp_size - 2)

    def span(j):
        return pl.ds(pl.multiple_of(j * cols, cols), cols)

    def direct(t, d, j):
        return pltpu.make_async_remote_copy(
            src_ref=inputs[t].at[0, :, span(j)],
            dst_ref=kv_buf.at[t, me, :, span(j)],
            send_sem=kv_send.at[t, d - 1],
            recv_sem=kv_recv.at[t, d - 1, j],
            device_id={"seq": far(d)},
            device_id_type=MESH,
        )

    def relay(t, d, j):
        block = kv_buf.at[t, source(d), :, span(j)]
        return pltpu.make_async_remote_copy(
            src_ref=block,
            dst_ref=block,
            send_sem=relay_send.at[t, d - 1],
            recv_sem=relay_recv.at[t, d - 1, j],
            device_id={"seq": partner},
            device_id_type=MESH,
        )

    def whole(t):
        return pltpu.make_async_remote_copy(
            src_ref=inputs[t].at[0],
            dst_ref=kv_buf.at[t, me],
            send_sem=pair_send.at[t],
            recv_sem=pair_recv.at[t],
            device_id={"seq": partner},
            device_id_type=MESH,
        )

    def send_chunk(j, carry):
        for d in range(1, chips):
            for t in range(2):
                direct(t, d, j).start()
        return carry

    send_chunk(0, 0)
    whole(0).start()
    whole(1).start()
    lax.fori_loop(1, chunk_count, send_chunk, 0)

    def relay_chunk(j):
        for d in range(1, chips):
            for t in range(2):
                direct(t, d, j).wait_recv()
                relay(t, d, j).start()

    for copy in locals_:
        copy.wait()
    for s in range(seq_size):
        taught_t[s * rows : (s + 1) * rows, :] = jnp.transpose(
            teacher_buf[:, s * rows : (s + 1) * rows].astype(jnp.float32)
        )
    cot_buf[...] = jnp.zeros_like(cot_buf)
    loss_acc[...] = jnp.zeros_like(loss_acc)

    heads = LANES // HEAD_DIM
    head_of_lane = lax.broadcasted_iota(jnp.int32, (rows, LANES), 1) // HEAD_DIM
    log2_scale = 1.0 / (math.sqrt(HEAD_DIM) * math.log(2.0))

    def attend(j):
        for d in range(1, chips):
            for t in range(2):
                relay(t, d, j).wait_recv()

        def group(p, carry):
            lanes = pl.ds(pl.multiple_of(j * cols + p * LANES, LANES), LANES)
            q = q_buf[:, lanes]
            stacked = jnp.concatenate(
                [jnp.where(head_of_lane == h, q, jnp.zeros_like(q)) for h in range(heads)], axis=0
            )
            k = kv_buf[0, :, :, lanes].reshape(tokens, LANES)
            v = kv_buf[1, :, :, lanes].reshape(tokens, LANES)
            scores = lax.dot_general(stacked, k, NT, preferred_element_type=jnp.float32)
            top = jnp.max(scores, axis=1, keepdims=True)
            weights = jnp.exp2((scores - top) * log2_scale)
            total = jnp.sum(weights, axis=1, keepdims=True)
            mixed = jnp.dot(weights.astype(jnp.bfloat16), v, preferred_element_type=jnp.float32)
            mixed = mixed * (1.0 / total)
            attended = mixed[:rows]
            for h in range(1, heads):
                attended = jnp.where(head_of_lane == h, mixed[h * rows : (h + 1) * rows], attended)
            attended = attended.astype(jnp.bfloat16).astype(jnp.float32)
            hat_buf[:, lanes] = stream_buf[:, lanes].astype(jnp.float32) + scale_buf[:, lanes] * attended
            return carry

        lax.fori_loop(0, cols // LANES, group, 0)

    relay_chunk(0)
    for t in range(2):
        whole(t).wait_recv()

    def attention_step(j, carry):
        relay_chunk(j)
        attend(j - 1)
        return carry

    lax.fori_loop(1, chunk_count, attention_step, 0)
    attend(chunk_count - 1)

    def part(r):
        return pl.ds(pl.multiple_of(r * slab, slab), slab)

    def fdirect(d, r):
        return pltpu.make_async_remote_copy(
            src_ref=feat_buf.at[me, part(r)],
            dst_ref=feat_buf.at[me, part(r)],
            send_sem=feat_send.at[d - 1, r],
            recv_sem=feat_recv.at[d - 1, r],
            device_id={"seq": far(d)},
            device_id_type=MESH,
        )

    def fpair(r):
        return pltpu.make_async_remote_copy(
            src_ref=feat_buf.at[me, part(r)],
            dst_ref=feat_buf.at[me, part(r)],
            send_sem=fpair_send.at[r],
            recv_sem=fpair_recv.at[r],
            device_id={"seq": partner},
            device_id_type=MESH,
        )

    def frelay(d, r):
        block = feat_buf.at[source(d), part(r)]
        return pltpu.make_async_remote_copy(
            src_ref=block,
            dst_ref=block,
            send_sem=frelay_send.at[d - 1, r],
            recv_sem=frelay_recv.at[d - 1, r],
            device_id={"seq": partner},
            device_id_type=MESH,
        )

    gain = gain_buf[...]

    def norm_slab(r, carry):
        here = part(r)
        summed = hat_buf[here, :]
        centred = summed - jnp.mean(summed, axis=1, keepdims=True)
        variance = jnp.mean(centred * centred, axis=1, keepdims=True)
        inv_sigma = lax.rsqrt(variance + EPSILON)
        hat = centred * inv_sigma
        normed = hat * gain
        inv_length = lax.rsqrt(jnp.sum(normed * normed, axis=1, keepdims=True) + EPSILON)
        feat_buf[me, here, :] = (normed * inv_length).astype(jnp.bfloat16)
        for d in range(1, chips):
            fdirect(d, r).start()
        fpair(r).start()
        hat_buf[here, :] = hat
        stats[0, here, :] = inv_sigma
        stats[1, here, :] = inv_length
        stats[2, here, :] = jnp.sum(normed * gain, axis=1, keepdims=True)
        return carry

    lax.fori_loop(0, slab_count, norm_slab, 0)

    def gram(s, start, size):
        block = feat_buf[s, pl.ds(start, size), :]
        tile = lax.dot_general(block, feat_buf[me], NT, preferred_element_type=jnp.float32)
        differ = tile - taught_t[pl.ds(pl.multiple_of(s * rows + start, size), size), :]
        loss_acc[...] += jnp.sum((differ * differ).reshape(size // 8, 8, rows), axis=0)
        cot_buf[...] += lax.dot_general(
            differ.astype(jnp.bfloat16), block, TN, preferred_element_type=jnp.float32
        )

    gram(me, 0, rows)
    for r in range(slab_count):
        fpair(r).wait_recv()
    gram(partner, 0, rows)

    def gram_step(i, carry):
        r = i // others
        d = lax.rem(i, others) + 1
        fdirect(d, r).wait_recv()
        frelay(d, r).start()
        start = pl.multiple_of(r * slab, slab)
        gram(source(d), start, slab)
        frelay(d, r).wait_recv()
        gram(source_pair(d), start, slab)
        return carry

    lax.fori_loop(0, others * slab_count, gram_step, 0)

    def lseq(i):
        return pltpu.make_async_remote_copy(
            src_ref=loss_seq.at[me],
            dst_ref=loss_seq.at[me],
            send_sem=lseq_send.at[i - 1],
            recv_sem=lseq_recv.at[i - 1],
            device_id={"seq": lax.rem(me + i, seq_size)},
            device_id_type=MESH,
        )

    def ldp(i):
        return pltpu.make_async_remote_copy(
            src_ref=loss_dp.at[image],
            dst_ref=loss_dp.at[image],
            send_sem=ldp_send.at[i - 1],
            recv_sem=ldp_recv.at[i - 1],
            device_id={"dp": lax.rem(image + i, dp_size)},
            device_id_type=MESH,
        )

    loss_seq[me] = loss_acc[...]
    for i in range(1, seq_size):
        lseq(i).start()

    inv_sigma = stats[0]
    inv_length = stats[1]
    cot_weight = 4.0 * width / (tokens * tokens)
    cot = cot_buf[...]
    along = cot_weight * jnp.sum(hat_buf[...] * gain * cot, axis=1, keepdims=True)
    gain_sum = cot_weight * jnp.sum(gain * cot, axis=1, keepdims=True)
    cubed = inv_length * inv_length * inv_length * along
    mean_scaled = (inv_length * gain_sum - cubed * stats[2]) * (1.0 / width)
    mean_product = cubed * (EPSILON / width)

    for i in range(1, seq_size):
        lseq(i).wait_recv()
    image_sum = loss_seq[0]
    for s in range(1, seq_size):
        image_sum = image_sum + loss_seq[s]
    loss_dp[image] = image_sum
    for i in range(1, dp_size):
        ldp(i).start()

    out_scale = inv_sigma * (tokens * math.sqrt(width))
    hat = hat_buf[...]
    scaled = (cot * (inv_length * cot_weight) - cubed * (hat * gain)) * gain
    grad_ref[0] = ((scaled - mean_scaled - hat * mean_product) * out_scale).astype(jnp.bfloat16)

    for i in range(1, dp_size):
        ldp(i).wait_recv()
    all_sum = loss_dp[0]
    for s in range(1, dp_size):
        all_sum = all_sum + loss_dp[s]
    loss_weight = width / (tokens * tokens)
    image_ref[0, 0] = jnp.sum(image_sum) * loss_weight
    mean_ref[0, 0] = jnp.sum(all_sum) * (loss_weight / dp_size)

    for t in range(2):
        whole(t).wait_send()
        for d in range(1, chips):
            pltpu.make_async_copy(inputs[t].at[0], kv_buf.at[t, me], kv_send.at[t, d - 1]).wait()
            pltpu.make_async_copy(inputs[t].at[0], kv_buf.at[t, me], relay_send.at[t, d - 1]).wait()
    for r in range(slab_count):
        fpair(r).wait_send()
        for d in range(1, chips):
            fdirect(d, r).wait_send()
            frelay(d, r).wait_send()
    for i in range(1, seq_size):
        lseq(i).wait_send()
    for i in range(1, dp_size):
        ldp(i).wait_send()


def local(seq_size, dp_size, queries, keys, values, stream, layer_scale, norm_gain, teacher_gram):
    rows, width = queries.shape[1:]
    others = max(1, seq_size // CORES - 1)
    tokens = rows * seq_size
    groups = width // LANES
    chunk_count = math.gcd(groups, max(1, 64 // seq_size))
    slab_count = max(1, rows // 32)
    dma = pltpu.SemaphoreType.DMA
    any_space = pl.BlockSpec(memory_space=pl.ANY)
    grad, image_loss, mean_loss = pl.pallas_call(
        functools.partial(kernel, seq_size, dp_size, chunk_count, slab_count),
        out_shape=(
            jax.ShapeDtypeStruct((1, rows, width), jnp.bfloat16),
            jax.ShapeDtypeStruct((1, 1), jnp.float32),
            jax.ShapeDtypeStruct((1, 1), jnp.float32),
        ),
        in_specs=[any_space] * 7,
        out_specs=(
            pl.BlockSpec(memory_space=pltpu.VMEM),
            pl.BlockSpec(memory_space=pltpu.SMEM),
            pl.BlockSpec(memory_space=pltpu.SMEM),
        ),
        scratch_shapes=[
            pltpu.VMEM((rows, width), jnp.bfloat16),
            pltpu.VMEM((2, seq_size, rows, width), jnp.bfloat16),
            pltpu.VMEM((rows, width), jnp.bfloat16),
            pltpu.VMEM((1, width), jnp.float32),
            pltpu.VMEM((1, width), jnp.float32),
            pltpu.VMEM((rows, tokens), jnp.bfloat16),
            pltpu.VMEM((tokens, rows), jnp.float32),
            pltpu.VMEM((rows, width), jnp.float32),
            pltpu.VMEM((seq_size, rows, width), jnp.bfloat16),
            pltpu.VMEM((rows, width), jnp.float32),
            pltpu.VMEM((3, rows, 1), jnp.float32),
            pltpu.VMEM((8, rows), jnp.float32),
            pltpu.VMEM((seq_size, 8, rows), jnp.float32),
            pltpu.VMEM((dp_size, 8, rows), jnp.float32),
            dma((7,)),
            dma((2, others)),
            dma((2, others, chunk_count)),
            dma((2,)),
            dma((2,)),
            dma((2, others)),
            dma((2, others, chunk_count)),
            dma((others, slab_count)),
            dma((others, slab_count)),
            dma((slab_count,)),
            dma((slab_count,)),
            dma((others, slab_count)),
            dma((others, slab_count)),
            dma((seq_size - 1,)),
            dma((seq_size - 1,)),
            dma((dp_size - 1,)),
            dma((dp_size - 1,)),
        ],
        compiler_params=pltpu.CompilerParams(
            collective_id=0, has_side_effects=True, vmem_limit_bytes=60 * 1024 * 1024
        ),
    )(
        queries,
        keys,
        values,
        stream,
        layer_scale.reshape(1, width),
        norm_gain.reshape(1, width),
        teacher_gram,
    )
    return grad, image_loss.reshape(1), mean_loss.reshape(())


def solution(mesh):
    return jax.shard_map(
        functools.partial(local, mesh.shape["seq"], mesh.shape["dp"]),
        mesh=mesh,
        in_specs=(
            P("dp", "seq", None),
            P("dp", "seq", None),
            P("dp", "seq", None),
            P("dp", "seq", None),
            P(),
            P(),
            P("dp", "seq", None),
        ),
        out_specs=(P("dp", "seq", None), P("dp"), P()),
        check_vma=False,
    )
```

```python
import functools
import math

import jax
import jax.numpy as jnp
from jax import lax
from jax.experimental import pallas as pl
from jax.experimental.pallas import tpu as pltpu
from jax.sharding import PartitionSpec as P

HEAD_DIM = 64
EPSILON = 1e-06
LANES = 128
CORES = 2
MESH = pl.DeviceIdType.MESH
NT = (((1,), (1,)), ((), ()))
TN = (((0,), (0,)), ((), ()))


def kernel(
    seq_size,
    dp_size,
    chunk_count,
    slab_count,
    q_hbm,
    k_hbm,
    v_hbm,
    stream_hbm,
    scale_hbm,
    gain_hbm,
    teacher_hbm,
    grad_ref,
    image_ref,
    mean_ref,
    q_buf,
    kv_buf,
    stream_buf,
    scale_buf,
    gain_buf,
    teacher_buf,
    taught_t,
    hat_buf,
    feat_buf,
    cot_buf,
    stats,
    loss_acc,
    loss_all,
    grad_buf,
    local_sem,
    kv_send,
    kv_recv,
    pair_send,
    pair_recv,
    relay_send,
    relay_recv,
    feat_send,
    feat_recv,
    fpair_send,
    fpair_recv,
    frelay_send,
    frelay_recv,
    loss_send,
    loss_recv,
    grad_sem,
    ready,
):
    rows, width = q_buf.shape
    chips = seq_size // CORES
    others = chips - 1
    tokens = rows * seq_size
    cols = width // chunk_count
    slab = rows // slab_count
    me = lax.axis_index("seq")
    image = lax.axis_index("dp")
    core = lax.rem(me, CORES)
    chip = me // CORES
    partner = chip * CORES + (1 - core)

    def far(d):
        return lax.rem(chip + d, chips) * CORES + core

    def source(d):
        return lax.rem(chip + chips - d, chips) * CORES + core

    def source_pair(d):
        return lax.rem(chip + chips - d, chips) * CORES + (1 - core)

    inputs = (k_hbm, v_hbm)
    locals_ = [
        pltpu.make_async_copy(src, dst, local_sem.at[i])
        for i, (src, dst) in enumerate(
            (
                (q_hbm.at[0], q_buf),
                (k_hbm.at[0], kv_buf.at[0, me]),
                (v_hbm.at[0], kv_buf.at[1, me]),
                (stream_hbm.at[0], stream_buf),
                (scale_hbm, scale_buf),
                (gain_hbm, gain_buf),
                (teacher_hbm.at[0], teacher_buf),
            )
        )
    ]

    barrier = pltpu.get_barrier_semaphore()

    def greet_seq(i, carry):
        pl.semaphore_signal(barrier, inc=1, device_id={"seq": lax.rem(me + i, seq_size)}, device_id_type=MESH)
        return carry

    lax.fori_loop(1, seq_size, greet_seq, 0)
    bits = dp_size.bit_length() - 1
    cube = dp_size == 1 << bits

    def across(k):
        return image + (1 << k) * (1 - 2 * lax.rem(image // (1 << k), 2))

    greeted = [across(k) for k in range(bits)] if cube else [lax.rem(image + i, dp_size) for i in range(1, dp_size)]
    for peer in greeted:
        pl.semaphore_signal(barrier, inc=1, device_id={"dp": peer}, device_id_type=MESH)
    for copy in locals_:
        copy.start()
    pl.semaphore_wait(barrier, seq_size - 1 + len(greeted))

    def span(j):
        return pl.ds(pl.multiple_of(j * cols, cols), cols)

    def direct(t, d, j):
        return pltpu.make_async_remote_copy(
            src_ref=inputs[t].at[0, :, span(j)],
            dst_ref=kv_buf.at[t, me, :, span(j)],
            send_sem=kv_send.at[t, d - 1],
            recv_sem=kv_recv.at[t, d - 1, j],
            device_id={"seq": far(d)},
            device_id_type=MESH,
        )

    def relay(t, d, j):
        block = kv_buf.at[t, source(d), :, span(j)]
        return pltpu.make_async_remote_copy(
            src_ref=block,
            dst_ref=block,
            send_sem=relay_send.at[t, d - 1],
            recv_sem=relay_recv.at[t, d - 1, j],
            device_id={"seq": partner},
            device_id_type=MESH,
        )

    def whole(t):
        return pltpu.make_async_remote_copy(
            src_ref=inputs[t].at[0],
            dst_ref=kv_buf.at[t, me],
            send_sem=pair_send.at[t],
            recv_sem=pair_recv.at[t],
            device_id={"seq": partner},
            device_id_type=MESH,
        )

    def send_chunk(j, carry):
        for d in range(1, chips):
            for t in range(2):
                direct(t, d, j).start()
        return carry

    send_chunk(0, 0)
    whole(0).start()
    whole(1).start()
    lax.fori_loop(1, chunk_count, send_chunk, 0)

    if cube:
        for k in range(bits):
            pl.semaphore_signal(ready.at[k], inc=1, device_id={"dp": across(k)}, device_id_type=MESH)
            pl.semaphore_wait(ready.at[k], 1)

    def relay_chunk(j):
        for d in range(1, chips):
            for t in range(2):
                direct(t, d, j).wait_recv()
                relay(t, d, j).start()

    for copy in locals_:
        copy.wait()
    for s in range(seq_size):
        taught_t[s * rows : (s + 1) * rows, :] = jnp.transpose(
            teacher_buf[:, s * rows : (s + 1) * rows].astype(jnp.float32)
        )
    cot_buf[...] = jnp.zeros_like(cot_buf)
    loss_acc[...] = jnp.zeros_like(loss_acc)

    heads = LANES // HEAD_DIM
    head_of_lane = lax.broadcasted_iota(jnp.int32, (rows, LANES), 1) // HEAD_DIM
    log2_scale = 1.0 / (math.sqrt(HEAD_DIM) * math.log(2.0))

    def attend(j):
        for d in range(1, chips):
            for t in range(2):
                relay(t, d, j).wait_recv()

        def group(p, carry):
            lanes = pl.ds(pl.multiple_of(j * cols + p * LANES, LANES), LANES)
            q = q_buf[:, lanes]
            stacked = jnp.concatenate(
                [jnp.where(head_of_lane == h, q, jnp.zeros_like(q)) for h in range(heads)], axis=0
            )
            k = kv_buf[0, :, :, lanes].reshape(tokens, LANES)
            v = kv_buf[1, :, :, lanes].reshape(tokens, LANES)
            scores = lax.dot_general(stacked, k, NT, preferred_element_type=jnp.float32)
            top = jnp.max(scores, axis=1, keepdims=True)
            weights = jnp.exp2((scores - top) * log2_scale)
            total = jnp.sum(weights, axis=1, keepdims=True)
            mixed = jnp.dot(weights.astype(jnp.bfloat16), v, preferred_element_type=jnp.float32)
            mixed = mixed * (1.0 / total)
            attended = mixed[:rows]
            for h in range(1, heads):
                attended = jnp.where(head_of_lane == h, mixed[h * rows : (h + 1) * rows], attended)
            attended = attended.astype(jnp.bfloat16).astype(jnp.float32)
            hat_buf[:, lanes] = stream_buf[:, lanes].astype(jnp.float32) + scale_buf[:, lanes] * attended
            return carry

        lax.fori_loop(0, cols // LANES, group, 0)

    relay_chunk(0)
    for t in range(2):
        whole(t).wait_recv()

    def attention_step(j, carry):
        relay_chunk(j)
        attend(j - 1)
        return carry

    lax.fori_loop(1, chunk_count, attention_step, 0)
    attend(chunk_count - 1)

    def part(r):
        return pl.ds(pl.multiple_of(r * slab, slab), slab)

    def fdirect(d, r):
        return pltpu.make_async_remote_copy(
            src_ref=feat_buf.at[me, part(r)],
            dst_ref=feat_buf.at[me, part(r)],
            send_sem=feat_send.at[d - 1, r],
            recv_sem=feat_recv.at[d - 1, r],
            device_id={"seq": far(d)},
            device_id_type=MESH,
        )

    def fpair(r):
        return pltpu.make_async_remote_copy(
            src_ref=feat_buf.at[me, part(r)],
            dst_ref=feat_buf.at[me, part(r)],
            send_sem=fpair_send.at[r],
            recv_sem=fpair_recv.at[r],
            device_id={"seq": partner},
            device_id_type=MESH,
        )

    def frelay(d, r):
        block = feat_buf.at[source(d), part(r)]
        return pltpu.make_async_remote_copy(
            src_ref=block,
            dst_ref=block,
            send_sem=frelay_send.at[d - 1, r],
            recv_sem=frelay_recv.at[d - 1, r],
            device_id={"seq": partner},
            device_id_type=MESH,
        )

    gain = gain_buf[...]

    def norm_slab(r, carry):
        here = part(r)
        summed = hat_buf[here, :]
        centred = summed - jnp.mean(summed, axis=1, keepdims=True)
        variance = jnp.mean(centred * centred, axis=1, keepdims=True)
        inv_sigma = lax.rsqrt(variance + EPSILON)
        hat = centred * inv_sigma
        normed = hat * gain
        inv_length = lax.rsqrt(jnp.sum(normed * normed, axis=1, keepdims=True) + EPSILON)
        feat_buf[me, here, :] = (normed * inv_length).astype(jnp.bfloat16)
        for d in range(1, chips):
            fdirect(d, r).start()
        fpair(r).start()
        hat_buf[here, :] = hat
        stats[0, here, :] = inv_sigma
        stats[1, here, :] = inv_length
        stats[2, here, :] = jnp.sum(normed * gain, axis=1, keepdims=True)
        return carry

    lax.fori_loop(0, slab_count, norm_slab, 0)

    def gram(s, start, size):
        block = feat_buf[s, pl.ds(start, size), :]
        tile = lax.dot_general(block, feat_buf[me], NT, preferred_element_type=jnp.float32)
        differ = tile - taught_t[pl.ds(pl.multiple_of(s * rows + start, size), size), :]
        loss_acc[...] += jnp.sum((differ * differ).reshape(size // 8, 8, rows), axis=0)
        return differ.astype(jnp.bfloat16)

    def pull(differ, s, start, size):
        block = feat_buf[s, pl.ds(start, size), :]
        cot_buf[...] += lax.dot_general(differ, block, TN, preferred_element_type=jnp.float32)

    pull(gram(me, 0, rows), me, 0, rows)
    for r in range(slab_count):
        fpair(r).wait_recv()
    pull(gram(partner, 0, rows), partner, 0, rows)

    def gram_step(i, finish):
        r = i // others
        d = lax.rem(i, others) + 1
        fdirect(d, r).wait_recv()
        frelay(d, r).start()
        start = pl.multiple_of(r * slab, slab)
        pull(gram(source(d), start, slab), source(d), start, slab)
        frelay(d, r).wait_recv()
        last = gram(source_pair(d), start, slab)
        finish()
        pull(last, source_pair(d), start, slab)

    def plain_step(i, carry):
        gram_step(i, lambda: None)
        return carry

    everyone = seq_size * dp_size
    mine = image * seq_size + me

    def send_loss():
        loss_all[mine] = jnp.sum(loss_acc[...], axis=0, keepdims=True)

        def tell(i, carry):
            target = lax.rem(mine + i, everyone)
            pltpu.make_async_remote_copy(
                src_ref=loss_all.at[mine],
                dst_ref=loss_all.at[mine],
                send_sem=loss_send,
                recv_sem=loss_recv,
                device_id={"dp": target // seq_size, "seq": lax.rem(target, seq_size)},
                device_id_type=MESH,
            ).start()
            return carry

        lax.fori_loop(1, everyone, tell, 0)

    if others:
        steps = others * slab_count
        lax.fori_loop(0, steps - 1, plain_step, 0)
        gram_step(steps - 1, send_loss)
    else:
        send_loss()

    inv_sigma = stats[0]
    inv_length = stats[1]
    cot_weight = 4.0 * width / (tokens * tokens)
    cot = cot_buf[...]
    along = cot_weight * jnp.sum(hat_buf[...] * gain * cot, axis=1, keepdims=True)
    gain_sum = cot_weight * jnp.sum(gain * cot, axis=1, keepdims=True)
    cubed = inv_length * inv_length * inv_length * along
    mean_scaled = (inv_length * gain_sum - cubed * stats[2]) * (1.0 / width)
    mean_product = cubed * (EPSILON / width)

    out_scale = inv_sigma * (tokens * math.sqrt(width))
    hat = hat_buf[...]
    scaled = (cot * (inv_length * cot_weight) - cubed * (hat * gain)) * gain
    grad_buf[...] = ((scaled - mean_scaled - hat * mean_product) * out_scale).astype(jnp.bfloat16)
    result = pltpu.make_async_copy(grad_buf, grad_ref.at[0], grad_sem)
    result.start()

    arrived = loss_all.at[pl.ds(0, everyone - 1)]
    pltpu.make_async_copy(arrived, arrived, loss_recv).wait()
    loss_weight = width / (tokens * tokens)
    image_ref[0, 0] = jnp.sum(loss_all[pl.ds(image * seq_size, seq_size)]) * loss_weight
    mean_ref[0, 0] = jnp.sum(loss_all[...]) * (loss_weight / dp_size)

    pltpu.make_async_copy(arrived, arrived, loss_send).wait()
    result.wait()
    for t in range(2):
        whole(t).wait_send()
        for d in range(1, chips):
            pltpu.make_async_copy(inputs[t].at[0], kv_buf.at[t, me], kv_send.at[t, d - 1]).wait()
            pltpu.make_async_copy(inputs[t].at[0], kv_buf.at[t, me], relay_send.at[t, d - 1]).wait()
    for r in range(slab_count):
        fpair(r).wait_send()
        for d in range(1, chips):
            fdirect(d, r).wait_send()
            frelay(d, r).wait_send()


def local(seq_size, dp_size, queries, keys, values, stream, layer_scale, norm_gain, teacher_gram):
    rows, width = queries.shape[1:]
    others = max(1, seq_size // CORES - 1)
    tokens = rows * seq_size
    groups = width // LANES
    chunk_count = math.gcd(groups, max(1, 64 // seq_size))
    slab_count = max(1, rows // 32)
    dma = pltpu.SemaphoreType.DMA
    any_space = pl.BlockSpec(memory_space=pl.ANY)
    grad, image_loss, mean_loss = pl.pallas_call(
        functools.partial(kernel, seq_size, dp_size, chunk_count, slab_count),
        out_shape=(
            jax.ShapeDtypeStruct((1, rows, width), jnp.bfloat16),
            jax.ShapeDtypeStruct((1, 1), jnp.float32),
            jax.ShapeDtypeStruct((1, 1), jnp.float32),
        ),
        in_specs=[any_space] * 7,
        out_specs=(
            any_space,
            pl.BlockSpec(memory_space=pltpu.SMEM),
            pl.BlockSpec(memory_space=pltpu.SMEM),
        ),
        scratch_shapes=[
            pltpu.VMEM((rows, width), jnp.bfloat16),
            pltpu.VMEM((2, seq_size, rows, width), jnp.bfloat16),
            pltpu.VMEM((rows, width), jnp.bfloat16),
            pltpu.VMEM((1, width), jnp.float32),
            pltpu.VMEM((1, width), jnp.float32),
            pltpu.VMEM((rows, tokens), jnp.bfloat16),
            pltpu.VMEM((tokens, rows), jnp.float32),
            pltpu.VMEM((rows, width), jnp.float32),
            pltpu.VMEM((seq_size, rows, width), jnp.bfloat16),
            pltpu.VMEM((rows, width), jnp.float32),
            pltpu.VMEM((3, rows, 1), jnp.float32),
            pltpu.VMEM((8, rows), jnp.float32),
            pltpu.VMEM((seq_size * dp_size, 1, rows), jnp.float32),
            pltpu.VMEM((rows, width), jnp.bfloat16),
            dma((7,)),
            dma((2, others)),
            dma((2, others, chunk_count)),
            dma((2,)),
            dma((2,)),
            dma((2, others)),
            dma((2, others, chunk_count)),
            dma((others, slab_count)),
            dma((others, slab_count)),
            dma((slab_count,)),
            dma((slab_count,)),
            dma((others, slab_count)),
            dma((others, slab_count)),
            dma,
            dma,
            dma,
            pltpu.SemaphoreType.REGULAR((max(1, dp_size.bit_length()),)),
        ],
        compiler_params=pltpu.CompilerParams(
            collective_id=0, has_side_effects=True, vmem_limit_bytes=60 * 1024 * 1024
        ),
    )(
        queries,
        keys,
        values,
        stream,
        layer_scale.reshape(1, width),
        norm_gain.reshape(1, width),
        teacher_gram,
    )
    return grad, image_loss.reshape(1), mean_loss.reshape(())


def solution(mesh):
    return jax.shard_map(
        functools.partial(local, mesh.shape["seq"], mesh.shape["dp"]),
        mesh=mesh,
        in_specs=(
            P("dp", "seq", None),
            P("dp", "seq", None),
            P("dp", "seq", None),
            P("dp", "seq", None),
            P(),
            P(),
            P("dp", "seq", None),
        ),
        out_specs=(P("dp", "seq", None), P("dp"), P()),
        check_vma=False,
    )
```

```python
import functools
import math

import jax
import jax.numpy as jnp
from jax import lax
from jax.experimental import pallas as pl
from jax.experimental.pallas import tpu as pltpu
from jax.sharding import PartitionSpec as P

HEAD_DIM = 64
EPSILON = 1e-06
LANES = 128
CORES = 2
MESH = pl.DeviceIdType.MESH
NT = (((1,), (1,)), ((), ()))
TN = (((0,), (0,)), ((), ()))


def kernel(
    seq_size,
    dp_size,
    chunk_count,
    slab_count,
    q_hbm,
    k_hbm,
    v_hbm,
    stream_hbm,
    scale_hbm,
    gain_hbm,
    teacher_hbm,
    grad_ref,
    image_ref,
    mean_ref,
    q_buf,
    kv_buf,
    stream_buf,
    scale_buf,
    gain_buf,
    teacher_buf,
    taught_t,
    hat_buf,
    feat_buf,
    cot_buf,
    diff_buf,
    stats,
    loss_acc,
    loss_all,
    grad_buf,
    local_sem,
    kv_send,
    kv_recv,
    pair_send,
    pair_recv,
    relay_send,
    relay_recv,
    feat_send,
    feat_recv,
    fpair_send,
    fpair_recv,
    frelay_send,
    frelay_recv,
    loss_send,
    loss_recv,
    grad_sem,
    ready,
):
    rows, width = q_buf.shape
    chips = seq_size // CORES
    others = chips - 1
    tokens = rows * seq_size
    cols = width // chunk_count
    slab = rows // slab_count
    me = lax.axis_index("seq")
    image = lax.axis_index("dp")
    core = lax.rem(me, CORES)
    chip = me // CORES
    partner = chip * CORES + (1 - core)

    def far(d):
        return lax.rem(chip + d, chips) * CORES + core

    def source(d):
        return lax.rem(chip + chips - d, chips) * CORES + core

    def source_pair(d):
        return lax.rem(chip + chips - d, chips) * CORES + (1 - core)

    inputs = (k_hbm, v_hbm)
    locals_ = [
        pltpu.make_async_copy(src, dst, local_sem.at[i])
        for i, (src, dst) in enumerate(
            (
                (q_hbm.at[0], q_buf),
                (k_hbm.at[0], kv_buf.at[0, me]),
                (v_hbm.at[0], kv_buf.at[1, me]),
                (stream_hbm.at[0], stream_buf),
                (scale_hbm, scale_buf),
                (gain_hbm, gain_buf),
                (teacher_hbm.at[0], teacher_buf),
            )
        )
    ]

    barrier = pltpu.get_barrier_semaphore()

    def greet_seq(i, carry):
        pl.semaphore_signal(barrier, inc=1, device_id={"seq": lax.rem(me + i, seq_size)}, device_id_type=MESH)
        return carry

    lax.fori_loop(1, seq_size, greet_seq, 0)
    bits = dp_size.bit_length() - 1
    cube = dp_size == 1 << bits

    def across(k):
        return image + (1 << k) * (1 - 2 * lax.rem(image // (1 << k), 2))

    greeted = [across(k) for k in range(bits)] if cube else [lax.rem(image + i, dp_size) for i in range(1, dp_size)]
    for peer in greeted:
        pl.semaphore_signal(barrier, inc=1, device_id={"dp": peer}, device_id_type=MESH)
    for copy in locals_:
        copy.start()
    pl.semaphore_wait(barrier, seq_size - 1 + len(greeted))

    def span(j):
        return pl.ds(pl.multiple_of(j * cols, cols), cols)

    def direct(t, d, j):
        return pltpu.make_async_remote_copy(
            src_ref=inputs[t].at[0, :, span(j)],
            dst_ref=kv_buf.at[t, me, :, span(j)],
            send_sem=kv_send.at[t, d - 1],
            recv_sem=kv_recv.at[t, d - 1, j],
            device_id={"seq": far(d)},
            device_id_type=MESH,
        )

    def relay(t, d, j):
        block = kv_buf.at[t, source(d), :, span(j)]
        return pltpu.make_async_remote_copy(
            src_ref=block,
            dst_ref=block,
            send_sem=relay_send.at[t, d - 1],
            recv_sem=relay_recv.at[t, d - 1, j],
            device_id={"seq": partner},
            device_id_type=MESH,
        )

    def whole(t):
        return pltpu.make_async_remote_copy(
            src_ref=inputs[t].at[0],
            dst_ref=kv_buf.at[t, me],
            send_sem=pair_send.at[t],
            recv_sem=pair_recv.at[t],
            device_id={"seq": partner},
            device_id_type=MESH,
        )

    def send_chunk(j, carry):
        for d in range(1, chips):
            for t in range(2):
                direct(t, d, j).start()
        return carry

    send_chunk(0, 0)
    whole(0).start()
    whole(1).start()
    lax.fori_loop(1, chunk_count, send_chunk, 0)

    if cube:
        for k in range(bits):
            pl.semaphore_signal(ready.at[k], inc=1, device_id={"dp": across(k)}, device_id_type=MESH)
            pl.semaphore_wait(ready.at[k], 1)

    def relay_chunk(j):
        for d in range(1, chips):
            for t in range(2):
                direct(t, d, j).wait_recv()
                relay(t, d, j).start()

    for copy in locals_:
        copy.wait()
    for s in range(seq_size):
        taught_t[s * rows : (s + 1) * rows, :] = jnp.transpose(
            teacher_buf[:, s * rows : (s + 1) * rows].astype(jnp.float32)
        )
    loss_acc[...] = jnp.zeros_like(loss_acc)

    heads = LANES // HEAD_DIM
    head_of_lane = lax.broadcasted_iota(jnp.int32, (rows, LANES), 1) // HEAD_DIM
    log2_scale = 1.0 / (math.sqrt(HEAD_DIM) * math.log(2.0))

    def attend(j):
        for d in range(1, chips):
            for t in range(2):
                relay(t, d, j).wait_recv()

        def group(p, carry):
            lanes = pl.ds(pl.multiple_of(j * cols + p * LANES, LANES), LANES)
            q = q_buf[:, lanes]
            stacked = jnp.concatenate(
                [jnp.where(head_of_lane == h, q, jnp.zeros_like(q)) for h in range(heads)], axis=0
            )
            k = kv_buf[0, :, :, lanes].reshape(tokens, LANES)
            v = kv_buf[1, :, :, lanes].reshape(tokens, LANES)
            scores = lax.dot_general(stacked, k, NT, preferred_element_type=jnp.float32)
            top = jnp.max(scores, axis=1, keepdims=True)
            weights = jnp.exp2((scores - top) * log2_scale)
            total = jnp.sum(weights, axis=1, keepdims=True)
            mixed = jnp.dot(weights.astype(jnp.bfloat16), v, preferred_element_type=jnp.float32)
            mixed = mixed * (1.0 / total)
            attended = mixed[:rows]
            for h in range(1, heads):
                attended = jnp.where(head_of_lane == h, mixed[h * rows : (h + 1) * rows], attended)
            attended = attended.astype(jnp.bfloat16).astype(jnp.float32)
            hat_buf[:, lanes] = stream_buf[:, lanes].astype(jnp.float32) + scale_buf[:, lanes] * attended
            return carry

        lax.fori_loop(0, cols // LANES, group, 0)

    relay_chunk(0)
    for t in range(2):
        whole(t).wait_recv()

    def attention_step(j, carry):
        relay_chunk(j)
        attend(j - 1)
        return carry

    lax.fori_loop(1, chunk_count, attention_step, 0)
    attend(chunk_count - 1)

    def part(r):
        return pl.ds(pl.multiple_of(r * slab, slab), slab)

    def fdirect(d, r):
        return pltpu.make_async_remote_copy(
            src_ref=feat_buf.at[me, part(r)],
            dst_ref=feat_buf.at[me, part(r)],
            send_sem=feat_send.at[d - 1, r],
            recv_sem=feat_recv.at[d - 1, r],
            device_id={"seq": far(d)},
            device_id_type=MESH,
        )

    def fpair(r):
        return pltpu.make_async_remote_copy(
            src_ref=feat_buf.at[me, part(r)],
            dst_ref=feat_buf.at[me, part(r)],
            send_sem=fpair_send.at[r],
            recv_sem=fpair_recv.at[r],
            device_id={"seq": partner},
            device_id_type=MESH,
        )

    def frelay(d, r):
        block = feat_buf.at[source(d), part(r)]
        return pltpu.make_async_remote_copy(
            src_ref=block,
            dst_ref=block,
            send_sem=frelay_send.at[d - 1, r],
            recv_sem=frelay_recv.at[d - 1, r],
            device_id={"seq": partner},
            device_id_type=MESH,
        )

    gain = gain_buf[...]

    def norm_slab(r, carry):
        here = part(r)
        summed = hat_buf[here, :]
        centred = summed - jnp.mean(summed, axis=1, keepdims=True)
        variance = jnp.mean(centred * centred, axis=1, keepdims=True)
        inv_sigma = lax.rsqrt(variance + EPSILON)
        hat = centred * inv_sigma
        normed = hat * gain
        inv_length = lax.rsqrt(jnp.sum(normed * normed, axis=1, keepdims=True) + EPSILON)
        feat_buf[me, here, :] = (normed * inv_length).astype(jnp.bfloat16)
        for d in range(1, chips):
            fdirect(d, r).start()
        fpair(r).start()
        hat_buf[here, :] = hat
        stats[0, here, :] = inv_sigma
        stats[1, here, :] = inv_length
        stats[2, here, :] = jnp.sum(normed * gain, axis=1, keepdims=True)
        return carry

    lax.fori_loop(0, slab_count, norm_slab, 0)

    def gram(s, start, size):
        block = feat_buf[s, pl.ds(start, size), :]
        tile = lax.dot_general(block, feat_buf[me], NT, preferred_element_type=jnp.float32)
        differ = tile - taught_t[pl.ds(pl.multiple_of(s * rows + start, size), size), :]
        loss_acc[...] += jnp.sum((differ * differ).reshape(size // 8, 8, rows), axis=0)
        diff_buf[s, pl.ds(start, size), :] = differ.astype(jnp.bfloat16)

    def pull(c):
        both = pl.ds(c * CORES, CORES)
        return lax.dot_general(
            diff_buf[both].reshape(CORES * rows, rows),
            feat_buf[both].reshape(CORES * rows, width),
            TN,
            preferred_element_type=jnp.float32,
        )

    gram(me, 0, rows)
    for r in range(slab_count):
        fpair(r).wait_recv()
    gram(partner, 0, rows)
    cot_buf[...] = pull(chip)

    def gram_step(i, carry):
        r = i // others
        d = lax.rem(i, others) + 1
        fdirect(d, r).wait_recv()
        frelay(d, r).start()
        start = pl.multiple_of(r * slab, slab)
        gram(source(d), start, slab)
        frelay(d, r).wait_recv()
        gram(source_pair(d), start, slab)
        return carry

    everyone = seq_size * dp_size
    mine = image * seq_size + me

    def send_loss():
        loss_all[mine] = jnp.sum(loss_acc[...], axis=0, keepdims=True)

        def tell(i, carry):
            target = lax.rem(mine + i, everyone)
            pltpu.make_async_remote_copy(
                src_ref=loss_all.at[mine],
                dst_ref=loss_all.at[mine],
                send_sem=loss_send,
                recv_sem=loss_recv,
                device_id={"dp": target // seq_size, "seq": lax.rem(target, seq_size)},
                device_id_type=MESH,
            ).start()
            return carry

        lax.fori_loop(1, everyone, tell, 0)

    lax.fori_loop(0, others * slab_count, gram_step, 0)
    send_loss()
    for d in range(1, chips):
        cot_buf[...] += pull(lax.rem(chip + d, chips))

    inv_sigma = stats[0]
    inv_length = stats[1]
    cot_weight = 4.0 * width / (tokens * tokens)
    cot = cot_buf[...]
    along = cot_weight * jnp.sum(hat_buf[...] * gain * cot, axis=1, keepdims=True)
    gain_sum = cot_weight * jnp.sum(gain * cot, axis=1, keepdims=True)
    cubed = inv_length * inv_length * inv_length * along
    mean_scaled = (inv_length * gain_sum - cubed * stats[2]) * (1.0 / width)
    mean_product = cubed * (EPSILON / width)

    out_scale = inv_sigma * (tokens * math.sqrt(width))
    hat = hat_buf[...]
    scaled = (cot * (inv_length * cot_weight) - cubed * (hat * gain)) * gain
    grad_buf[...] = ((scaled - mean_scaled - hat * mean_product) * out_scale).astype(jnp.bfloat16)
    result = pltpu.make_async_copy(grad_buf, grad_ref.at[0], grad_sem)
    result.start()

    arrived = loss_all.at[pl.ds(0, everyone - 1)]
    pltpu.make_async_copy(arrived, arrived, loss_recv).wait()
    loss_weight = width / (tokens * tokens)
    image_ref[0, 0] = jnp.sum(loss_all[pl.ds(image * seq_size, seq_size)]) * loss_weight
    mean_ref[0, 0] = jnp.sum(loss_all[...]) * (loss_weight / dp_size)

    pltpu.make_async_copy(arrived, arrived, loss_send).wait()
    result.wait()
    for t in range(2):
        whole(t).wait_send()
        for d in range(1, chips):
            pltpu.make_async_copy(inputs[t].at[0], kv_buf.at[t, me], kv_send.at[t, d - 1]).wait()
            pltpu.make_async_copy(inputs[t].at[0], kv_buf.at[t, me], relay_send.at[t, d - 1]).wait()
    for r in range(slab_count):
        fpair(r).wait_send()
        for d in range(1, chips):
            fdirect(d, r).wait_send()
            frelay(d, r).wait_send()


def local(seq_size, dp_size, queries, keys, values, stream, layer_scale, norm_gain, teacher_gram):
    rows, width = queries.shape[1:]
    others = max(1, seq_size // CORES - 1)
    tokens = rows * seq_size
    groups = width // LANES
    chunk_count = math.gcd(groups, max(1, 64 // seq_size))
    slab_count = max(1, rows // 32)
    dma = pltpu.SemaphoreType.DMA
    any_space = pl.BlockSpec(memory_space=pl.ANY)
    grad, image_loss, mean_loss = pl.pallas_call(
        functools.partial(kernel, seq_size, dp_size, chunk_count, slab_count),
        out_shape=(
            jax.ShapeDtypeStruct((1, rows, width), jnp.bfloat16),
            jax.ShapeDtypeStruct((1, 1), jnp.float32),
            jax.ShapeDtypeStruct((1, 1), jnp.float32),
        ),
        in_specs=[any_space] * 7,
        out_specs=(
            any_space,
            pl.BlockSpec(memory_space=pltpu.SMEM),
            pl.BlockSpec(memory_space=pltpu.SMEM),
        ),
        scratch_shapes=[
            pltpu.VMEM((rows, width), jnp.bfloat16),
            pltpu.VMEM((2, seq_size, rows, width), jnp.bfloat16),
            pltpu.VMEM((rows, width), jnp.bfloat16),
            pltpu.VMEM((1, width), jnp.float32),
            pltpu.VMEM((1, width), jnp.float32),
            pltpu.VMEM((rows, tokens), jnp.bfloat16),
            pltpu.VMEM((tokens, rows), jnp.float32),
            pltpu.VMEM((rows, width), jnp.float32),
            pltpu.VMEM((seq_size, rows, width), jnp.bfloat16),
            pltpu.VMEM((rows, width), jnp.float32),
            pltpu.VMEM((seq_size, rows, rows), jnp.bfloat16),
            pltpu.VMEM((3, rows, 1), jnp.float32),
            pltpu.VMEM((8, rows), jnp.float32),
            pltpu.VMEM((seq_size * dp_size, 1, rows), jnp.float32),
            pltpu.VMEM((rows, width), jnp.bfloat16),
            dma((7,)),
            dma((2, others)),
            dma((2, others, chunk_count)),
            dma((2,)),
            dma((2,)),
            dma((2, others)),
            dma((2, others, chunk_count)),
            dma((others, slab_count)),
            dma((others, slab_count)),
            dma((slab_count,)),
            dma((slab_count,)),
            dma((others, slab_count)),
            dma((others, slab_count)),
            dma,
            dma,
            dma,
            pltpu.SemaphoreType.REGULAR((max(1, dp_size.bit_length()),)),
        ],
        compiler_params=pltpu.CompilerParams(
            collective_id=0, has_side_effects=True, vmem_limit_bytes=60 * 1024 * 1024
        ),
    )(
        queries,
        keys,
        values,
        stream,
        layer_scale.reshape(1, width),
        norm_gain.reshape(1, width),
        teacher_gram,
    )
    return grad, image_loss.reshape(1), mean_loss.reshape(())


def solution(mesh):
    return jax.shard_map(
        functools.partial(local, mesh.shape["seq"], mesh.shape["dp"]),
        mesh=mesh,
        in_specs=(
            P("dp", "seq", None),
            P("dp", "seq", None),
            P("dp", "seq", None),
            P("dp", "seq", None),
            P(),
            P(),
            P("dp", "seq", None),
        ),
        out_specs=(P("dp", "seq", None), P("dp"), P()),
        check_vma=False,
    )
```
